32 devices in a mesh: rep: 1, dp: 32 (over x, y, z, core).
Axes of the slice: x: 2, y: 2, z: 4, core: 2. Of those that a mesh axis runs over, the one named last changes fastest.
Arguments:
- x: bfloat16 [32, 2048, 1024], P(('rep', 'dp'))
- dy: bfloat16 [32, 2048, 1024], P(('rep', 'dp'))
- w_gate: bfloat16 [2, 1024, 5120], replicated
- w_up: bfloat16 [2, 1024, 5120], replicated
- w_down: bfloat16 [2, 5120, 1024], replicated
- m_w_gate: float32 [2, 1024, 5120], P(None, 'dp')
- m_w_up: float32 [2, 1024, 5120], P(None, 'dp')
- m_w_down: float32 [2, 5120, 1024], P(None, 'dp')
- v_w_gate: float32 [2, 1024, 5120], P(None, 'dp')
- v_w_up: float32 [2, 1024, 5120], P(None, 'dp')
- v_w_down: float32 [2, 5120, 1024], P(None, 'dp')
Outputs:
- output 1: bfloat16 [2, 1024, 5120], P('rep')
- output 2: bfloat16 [2, 1024, 5120], P('rep')
- output 3: bfloat16 [2, 5120, 1024], P('rep')
- output 4: float32 [2, 1024, 5120], P('rep', 'dp')
- output 5: float32 [2, 1024, 5120], P('rep', 'dp')
- output 6: float32 [2, 5120, 1024], P('rep', 'dp')
- output 7: float32 [2, 1024, 5120], P('rep', 'dp')
- output 8: float32 [2, 1024, 5120], P('rep', 'dp')
- output 9: float32 [2, 5120, 1024], P('rep', 'dp')
All inputs are finite; a program needn't handle non-finite values.
Results may differ from the reference program's by a relative error of at most 0.022.
Values are sent between devices in bfloat16 or wider.
A program may use at most 2 GiB of HBM per device.

```python
import jax
import jax.numpy as jnp
from jax import lax

SEQUENCES = 32
TOKENS = 2048
D = 1024
FF = 5120
LAYERS = 2
NAMES = ("w_gate", "w_up", "w_down")
SHAPES = {"w_gate": (LAYERS, D, FF), "w_up": (LAYERS, D, FF), "w_down": (LAYERS, FF, D)}


def bump(key, n, height):
    away = (jnp.arange(n, dtype=jnp.int32) - jax.random.randint(key, (), 0, n, jnp.int32)) % n
    return jnp.where(away < n // 8, height, 1.0)


def together(key, own, strength):
    shared = jax.random.normal(key, own.shape[1:], jnp.float32)
    return (own + strength * shared) * lax.rsqrt(1 + strength * strength)


def setup_inputs(seed: int = 0, part: int = 0) -> dict:
    kx, kdy, ka, kb, kz, kf, kh, kl, *keys = jax.random.split(jax.random.key(seed), 8 + 3 * len(NAMES))
    kx, kdy, ka, kb = (jax.random.fold_in(k, part) for k in (kx, kdy, ka, kb))
    kw, km, kv = (keys[i::3] for i in range(3))
    shape = (SEQUENCES, TOKENS, D)
    much_x, much_dy = jax.random.uniform(kz, (2,), jnp.float32, 0.0, 1.0)
    loud = 2.0 ** jax.random.uniform(jax.random.fold_in(kz, 1), (), jnp.float32, -1.0, 2.0)
    layers = 2.0 ** jax.random.uniform(kl, (LAYERS, 1, 1), jnp.float32, -1.0, 1.0)
    x = together(ka, jax.random.normal(kx, shape, jnp.float32), much_x) * bump(kf, D, 4.0)
    dy = together(kb, jax.random.normal(kdy, shape, jnp.float32), much_dy)
    drawn = {"x": x.astype(jnp.bfloat16), "dy": (loud * dy * (SEQUENCES * TOKENS) ** -0.5).astype(jnp.bfloat16)}
    for key, name in zip(kw, NAMES, strict=True):
        w = jax.random.normal(key, SHAPES[name], jnp.float32) * SHAPES[name][1] ** -0.5
        drawn[name] = (w * {"w_gate": 1.0, "w_up": bump(kh, FF, 4.0), "w_down": layers}[name]).astype(jnp.bfloat16)
    for key, name in zip(km, NAMES, strict=True):
        drawn[f"m_{name}"] = 0.1 * jax.random.normal(key, SHAPES[name], jnp.float32)
    for key, name in zip(kv, NAMES, strict=True):
        drawn[f"v_{name}"] = jax.random.uniform(key, SHAPES[name], jnp.float32, 0.005, 0.015)
    return drawn


def matmul(a, w):
    return jnp.dot(a, w, preferred_element_type=jnp.float32).astype(jnp.bfloat16)


def normed(h):
    wide = h.astype(jnp.float32)
    scale = lax.rsqrt(jnp.mean(wide**2, -1, keepdims=True) + 1e-6)
    return (wide * scale).astype(jnp.bfloat16)


def layer(h, w):
    a = normed(h)
    gate = jnp.dot(a, w["w_gate"], preferred_element_type=jnp.float32)
    up = jnp.dot(a, w["w_up"], preferred_element_type=jnp.float32)
    return h + matmul((jax.nn.silu(gate) * up).astype(jnp.bfloat16), w["w_down"])


def adamw(w, m, v, g):
    m = 0.9 * m + 0.1 * g
    v = 0.95 * v + 0.05 * g * g
    step = m * lax.rsqrt(v + 1e-8) + 0.1 * w
    return (w - 0.02 * step).astype(jnp.bfloat16), m, v


def stack(weights, h):
    return lax.scan(lambda h, w: (layer(h, w), None), h, weights)[0]


def reference(x, dy, w_gate, w_up, w_down, m_w_gate, m_w_up, m_w_down, v_w_gate, v_w_up, v_w_down):
    weights = dict(zip(NAMES, (w_gate, w_up, w_down), strict=True))

    def take(so_far, sequence):
        h, by_y = sequence
        _, back = jax.vjp(lambda w: stack(w, h), weights)
        return jax.tree.map(lambda total, term: total + term.astype(jnp.float32), so_far, back(by_y)[0]), None

    none_yet = {name: jnp.zeros(w.shape, jnp.float32) for name, w in weights.items()}
    by_weights, _ = lax.scan(take, none_yet, (x, dy))
    gradients = [by_weights[name].astype(jnp.bfloat16).astype(jnp.float32) for name in NAMES]
    new = [
        adamw(w.astype(jnp.float32), m, v, g)
        for w, m, v, g in zip((w_gate, w_up, w_down), (m_w_gate, m_w_up, m_w_down), (v_w_gate, v_w_up, v_w_down), gradients, strict=True)
    ]
    return tuple(one[which] for which in range(3) for one in new)
```

```python
import jax
import jax.numpy as jnp
from jax import lax
from jax.sharding import PartitionSpec as P

NAMES = ("w_gate", "w_up", "w_down")


def matmul(a, w):
    return jnp.dot(a, w, preferred_element_type=jnp.float32).astype(jnp.bfloat16)


def normed(h):
    wide = h.astype(jnp.float32)
    scale = lax.rsqrt(jnp.mean(wide**2, -1, keepdims=True) + 1e-6)
    return (wide * scale).astype(jnp.bfloat16)


def layer(h, w):
    a = normed(h)
    gate = jnp.dot(a, w["w_gate"], preferred_element_type=jnp.float32)
    up = jnp.dot(a, w["w_up"], preferred_element_type=jnp.float32)
    return h + matmul((jax.nn.silu(gate) * up).astype(jnp.bfloat16), w["w_down"])


def adamw(w, m, v, g):
    m = 0.9 * m + 0.1 * g
    v = 0.95 * v + 0.05 * g * g
    step = m * lax.rsqrt(v + 1e-8) + 0.1 * w
    return (w - 0.02 * step).astype(jnp.bfloat16), m, v


def solution(mesh):
    def step(x, dy, *arrays):
        weights, m, v = (arrays[i : i + 3] for i in (0, 3, 6))
        x, dy = x[0], dy[0]
        layers = weights[0].shape[0]
        per_layer = [{name: w[number] for name, w in zip(NAMES, weights, strict=True)} for number in range(layers)]

        def stack(per_layer):
            h = x
            for w in per_layer:
                h = layer(h, w)
            return h

        _, back = jax.vjp(stack, per_layer)
        grads = back(dy)[0]
        me = lax.axis_index("dp")
        new = {name: [None] * layers for name in NAMES}
        for number in reversed(range(layers)):
            for i, name in reversed(list(enumerate(NAMES))):
                g = lax.psum_scatter(grads[number][name], "dp", scatter_dimension=0, tiled=True)
                rows = g.shape[0]
                w = lax.dynamic_slice_in_dim(weights[i][number], me * rows, rows, 0)
                w, nm, nv = adamw(w.astype(jnp.float32), m[i][number], v[i][number], g.astype(jnp.float32))
                new[name][number] = (lax.all_gather(w, "dp", axis=0, tiled=True), nm, nv)
        return tuple(jnp.stack([new[name][number][which] for number in range(layers)]) for which in range(3) for name in NAMES)

    whole, rows, seq = P(None, None, None), P(None, "dp", None), P(("rep", "dp"), None, None)
    return jax.shard_map(
        step,
        mesh=mesh,
        in_specs=(seq, seq) + (whole,) * 3 + (rows,) * 6,
        out_specs=(P("rep", None, None),) * 3 + (P("rep", "dp", None),) * 6,
        check_vma=False,
    )
```

```python
import functools
import jax, jax.numpy as jnp
from jax import lax
from jax.experimental import pallas as pl
from jax.experimental.pallas import tpu as pltpu
from jax.sharding import PartitionSpec as P

MESH = pl.DeviceIdType.MESH
f32, bf16 = jnp.float32, jnp.bfloat16

def idx(x, y, z, c):
    return ((x * 2 + y) * 4 + z) * 2 + c

class Me:
    def __init__(self):
        d = lax.axis_index("dp")
        self.c = lax.rem(d, 2)
        self.z = lax.rem(lax.div(d, 2), 4)
        self.y = lax.rem(lax.div(d, 8), 2)
        self.x = lax.div(d, 16)
    def core(self): return idx(self.x, self.y, self.z, 1 - self.c)
    def xn(self): return idx(1 - self.x, self.y, self.z, self.c)
    def yn(self): return idx(self.x, 1 - self.y, self.z, self.c)
    def zk(self, k): return idx(self.x, self.y, lax.rem(self.z + k, 4), self.c)

def barrier(me):
    sem = pltpu.get_barrier_semaphore()
    peers = [me.core(), me.xn(), me.yn()] + [me.zk(k) for k in (1, 2, 3)]
    for p in peers:
        pl.semaphore_signal(sem, inc=1, device_id={"dp": p}, device_id_type=MESH)
    pl.semaphore_wait(sem, len(peers))

def sel(k, a, b):
    return (1 - k) * a + k * b

class Sems:
    def __init__(self, send, recv):
        self.send, self.recv, self.n = send, recv, 0
    def copy(self, src, dst, dev):
        i = self.n; self.n += 1
        return pltpu.make_async_remote_copy(src_ref=src, dst_ref=dst, send_sem=self.send.at[i], recv_sem=self.recv.at[i],
                                            device_id={"dp": dev}, device_id_type=MESH)
SEMS_PER = 19

class Unit:
    def __init__(self, me, sems, layer, r, C, G, Wold, m, v, Wnew, mo, vo, bufs):
        self.me, self.sems, self.l, self.r, self.C = me, sems, layer, r, C
        self.G, self.Wold, self.m, self.v, self.W, self.mo, self.vo = G, Wold, m, v, Wnew, mo, vo
        self.R0, self.S0, self.R1, self.S1, self.R2, self.S2, self.R3 = bufs
        self.pending = []
        self.cp = {}
    def start(self, key, cps):
        self.cp[key] = cps
        for c in cps: c.start()
    def wait(self, key):
        for c in self.cp[key]: c.wait_recv()
    def drain(self):
        for cps in self.cp.values():
            for c in cps: c.wait_send()
    def s0(self):
        me, s = self.me, self.sems
        cps = []
        for x in range(2):
            for y in range(2):
                cps.append(s.copy(self.G.at[x, y, :, 1 - me.c], self.R0.at[x, y], me.core()))
        self.start("core", cps)
    def s1(self):
        me, h, C = self.me, self.r // 2, self.C
        x, y, z, c = me.x, me.y, me.z, me.c
        self.wait("core")
        def xyz(k, j): return sel(k, 1 - x, j // 4), sel(k, j // 4, 1 - y), j % 4
        def gm(k, j):
            a, b, d = xyz(k, j); return (a, b, d, c, k, 0)
        def rm(k, j):
            a, b, d = xyz(k, j); return (a, b, d, k, 0)
        def body(g, r0, o):
            o[...] = (g[...].astype(f32) + r0[...].astype(f32)).astype(bf16)
        N = None
        pltpu.emit_pipeline(body, grid=(2, 8),
            in_specs=[pl.BlockSpec((N, N, N, N, h, C), gm), pl.BlockSpec((N, N, N, h, C), rm)],
            out_specs=[pl.BlockSpec((N, N, h, C), lambda k, j: (k, j, 0, 0))])(self.G, self.R0, self.S0)
        self.start("xy1", [self.sems.copy(self.S0.at[0], self.R1.at[0], me.xn()), self.sems.copy(self.S0.at[1], self.R1.at[1], me.yn())])
    def s2(self):
        me, h, C = self.me, self.r // 2, self.C
        x, y, z, c = me.x, me.y, me.z, me.c
        self.wait("xy1")
        def gm(k, j): return (sel(k, x, 1 - x), sel(k, 1 - y, y), j, c, k, 0)
        def rm(k, j): return (sel(k, x, 1 - x), sel(k, 1 - y, y), j, k, 0)
        def r1(k, j): return (k, sel(k, 1 - y, 1 - x) * 4 + j, 0, 0)
        def body(g, r0, r1, o):
            o[...] = (g[...].astype(f32) + r0[...].astype(f32) + r1[...].astype(f32)).astype(bf16)
        N = None
        pltpu.emit_pipeline(body, grid=(2, 4),
            in_specs=[pl.BlockSpec((N, N, N, N, h, C), gm), pl.BlockSpec((N, N, N, h, C), rm), pl.BlockSpec((N, N, h, C), r1)],
            out_specs=[pl.BlockSpec((N, N, h, C), lambda k, j: (k, j, 0, 0))])(self.G, self.R0, self.R1, self.S1)
        self.start("xy2", [self.sems.copy(self.S1.at[0], self.R2.at[0], me.yn()), self.sems.copy(self.S1.at[1], self.R2.at[1], me.xn())])
    def s3(self):
        me, h, C = self.me, self.r // 2, self.C
        x, y, z, c = me.x, me.y, me.z, me.c
        self.wait("xy2")
        def zz(j): return lax.rem(z + 1 + j, 4)
        def gm(j, k): return (x, y, zz(j), c, k, 0)
        def rm(j, k): return (x, y, zz(j), k, 0)
        def r1(j, k): return (k, sel(k, y, x) * 4 + zz(j), 0, 0)
        def r2(j, k): return (k, zz(j), 0, 0)
        def body(g, r0, r1, r2, o):
            o[...] = (g[...].astype(f32) + r0[...].astype(f32) + r1[...].astype(f32) + r2[...].astype(f32)).astype(bf16)
        N = None
        pltpu.emit_pipeline(body, grid=(3, 2),
            in_specs=[pl.BlockSpec((N, N, N, N, h, C), gm), pl.BlockSpec((N, N, N, h, C), rm), pl.BlockSpec((N, N, h, C), r1), pl.BlockSpec((N, N, h, C), r2)],
            out_specs=[pl.BlockSpec((N, h, C), lambda j, k: (j, k, 0))])(self.G, self.R0, self.R1, self.R2, self.S2)
        self.start("z", [self.sems.copy(self.S2.at[k - 1], self.R3.at[k - 1], me.zk(k)) for k in (1, 2, 3)])
    def s4(self):
        me, h, C, l = self.me, self.r // 2, self.C, self.l
        x, y, z, c = me.x, me.y, me.z, me.c
        self.wait("z")
        N = None
        def body(g, r0, r1, r2, r3, w, m, v, wo, mo, vo):
            t = g[...].astype(f32) + r0[...].astype(f32) + r1[...].astype(f32) + r2[...].astype(f32)
            for k in range(3): t = t + r3[k].astype(f32)
            t = t.astype(bf16).astype(f32)
            mm = 0.9 * m[...] + 0.1 * t
            vv = 0.95 * v[...] + 0.05 * t * t
            ww = w[...].astype(f32)
            step = mm * lax.rsqrt(vv + 1e-8) + 0.1 * ww
            wo[...] = (ww - 0.02 * step).astype(bf16)
            mo[...] = mm
            vo[...] = vv
        wspec = pl.BlockSpec((N, N, N, N, N, h, C), lambda k: (l, x, y, z, c, k, 0))
        mspec = pl.BlockSpec((N, h, C), lambda k: (l, k, 0))
        pltpu.emit_pipeline(body, grid=(2,),
            in_specs=[pl.BlockSpec((N, N, N, N, h, C), lambda k: (x, y, z, c, k, 0)), pl.BlockSpec((N, N, N, h, C), lambda k: (x, y, z, k, 0)),
                      pl.BlockSpec((N, N, h, C), lambda k: (k, sel(k, y, x) * 4 + z, 0, 0)), pl.BlockSpec((N, N, h, C), lambda k: (k, z, 0, 0)),
                      pl.BlockSpec((3, h, C), lambda k: (0, k, 0)), wspec, mspec, mspec],
            out_specs=[wspec, mspec, mspec])(self.G, self.R0, self.R1, self.R2, self.R3, self.Wold, self.m, self.v, self.W, self.mo, self.vo)
        src = self.W.at[l, x, y, z, c]
        self.start("az", [self.sems.copy(src, src, me.zk(k)) for k in (1, 2, 3)])
    def g1(self):
        me, h, l = self.me, self.r // 2, self.l
        x, y, z, c = me.x, me.y, me.z, me.c
        self.wait("az")
        A = self.W.at[l, x, y, :, c, pl.ds(0, h)]; B = self.W.at[l, x, y, :, c, pl.ds(h, h)]
        self.start("axy1", [self.sems.copy(A, A, me.yn()), self.sems.copy(B, B, me.xn())])
        F = self.W.at[l, x, y, :, c]
        self.start("ac0", [self.sems.copy(F, F, me.core())])
    def g2(self):
        me, h, l = self.me, self.r // 2, self.l
        x, y, z, c = me.x, me.y, me.z, me.c
        self.wait("axy1")
        cps = []
        for q in range(2):
            A = self.W.at[l, x, q, :, c, pl.ds(0, h)]; B = self.W.at[l, q, y, :, c, pl.ds(h, h)]
            cps += [self.sems.copy(A, A, me.xn()), self.sems.copy(B, B, me.yn())]
        self.start("axy2", cps)
        A = self.W.at[l, x, 1 - y, :, c, pl.ds(0, h)]; B = self.W.at[l, 1 - x, y, :, c, pl.ds(h, h)]
        self.start("ac1", [self.sems.copy(A, A, me.core()), self.sems.copy(B, B, me.core())])
    def g3(self):
        me, h, l = self.me, self.r // 2, self.l
        x, y, z, c = me.x, me.y, me.z, me.c
        self.wait("axy2")
        cps = []
        for q in range(2):
            A = self.W.at[l, 1 - x, q, :, c, pl.ds(0, h)]; B = self.W.at[l, q, 1 - y, :, c, pl.ds(h, h)]
            cps += [self.sems.copy(A, A, me.core()), self.sems.copy(B, B, me.core())]
        self.start("ac2", cps)
    def g4(self):
        for k in ("ac0", "ac1", "ac2"): self.wait(k)
        self.drain()

def buf_shapes(r, C):
    h = r // 2
    S = lambda *s: jax.ShapeDtypeStruct(s, bf16)
    return [S(2, 2, 4, r, C), S(2, 8, h, C), S(2, 8, h, C), S(2, 4, h, C), S(2, 4, h, C), S(3, r, C), S(3, r, C)]
NB = 7


NAMES = ("w_gate", "w_up", "w_down")
ORDER = ((1, 2), (1, 0), (1, 1), (0, 2), (0, 0), (0, 1))
STAGES = ("s0", "s1", "s2", "s3", "s4", "g1", "g2", "g3", "g4")


def matmul(a, w):
    return jnp.dot(a, w, preferred_element_type=jnp.float32).astype(jnp.bfloat16)


def normed(h):
    wide = h.astype(jnp.float32)
    scale = lax.rsqrt(jnp.mean(wide**2, -1, keepdims=True) + 1e-6)
    return (wide * scale).astype(jnp.bfloat16)


def layer(h, w):
    a = normed(h)
    gate = jnp.dot(a, w["w_gate"], preferred_element_type=jnp.float32)
    up = jnp.dot(a, w["w_up"], preferred_element_type=jnp.float32)
    return h + matmul((jax.nn.silu(gate) * up).astype(jnp.bfloat16), w["w_down"])


def skew_order(count, lag):
    order = []
    for t in range(lag * count + len(STAGES)):
        for u in range(count):
            if 0 <= t - lag * u < len(STAGES):
                order.append((u, STAGES[t - lag * u]))
    return order


def kernel(sizes, order, *refs):
    n = len(ORDER)
    G, Wold, M, V, o = refs[:n], refs[n : n + 3], refs[n + 3 : n + 6], refs[n + 6 : n + 9], refs[n + 9 :]
    Wn, Mo, Vo, bufs, (ssem, rsem) = o[:3], o[3:6], o[6:9], o[9 : 9 + NB * n], o[9 + NB * n :]
    me = Me()
    barrier(me)
    sems = Sems(ssem, rsem)
    units = [
        Unit(me, sems, l, *sizes[w], G[i], Wold[w], M[w], V[w], Wn[w], Mo[w], Vo[w], bufs[NB * i : NB * i + NB])
        for i, (l, w) in enumerate(ORDER)
    ]
    for u, s in order:
        getattr(units[u], s)()


def communicate(sizes, layers, *args):
    hbm = pl.BlockSpec(memory_space=pl.ANY)
    outs = [jax.ShapeDtypeStruct((layers, 2, 2, 4, 2, r, C), bf16) for r, C in sizes]
    outs += [jax.ShapeDtypeStruct((layers, r, C), f32) for r, C in sizes] * 2
    for _, w in ORDER:
        outs += buf_shapes(*sizes[w])
    count = 27 * len(ORDER)
    return pl.pallas_call(
        functools.partial(kernel, sizes, skew_order(len(ORDER), 1)),
        out_shape=outs,
        in_specs=[hbm] * len(args),
        out_specs=[hbm] * len(outs),
        scratch_shapes=[pltpu.SemaphoreType.DMA((count,)), pltpu.SemaphoreType.DMA((count,))],
        compiler_params=pltpu.CompilerParams(collective_id=0, has_side_effects=True, vmem_limit_bytes=60 << 20),
    )(*args)


def solution(mesh):
    def step(x, dy, *arrays):
        weights, m, v = (arrays[i : i + 3] for i in (0, 3, 6))
        x, dy = x[0], dy[0]
        layers = weights[0].shape[0]
        sizes = [t.shape[1:] for t in m]
        per_layer = [{name: w[number] for name, w in zip(NAMES, weights, strict=True)} for number in range(layers)]

        def stack(per_layer):
            h = x
            for w in per_layer:
                h = layer(h, w)
            return h

        _, back = jax.vjp(stack, per_layer)
        grads = back(dy)[0]
        gs = [grads[l][NAMES[w]].reshape(2, 2, 4, 2, *sizes[w]) for l, w in ORDER]
        ws = [w.reshape(layers, 2, 2, 4, 2, *s) for w, s in zip(weights, sizes, strict=True)]
        out = communicate(sizes, layers, *gs, *ws, *m, *v)
        return tuple(w.reshape(t.shape) for w, t in zip(out[:3], weights, strict=True)) + tuple(out[3:9])

    whole, rows, seq = P(None, None, None), P(None, "dp", None), P(("rep", "dp"), None, None)
    return jax.shard_map(
        step,
        mesh=mesh,
        in_specs=(seq, seq) + (whole,) * 3 + (rows,) * 6,
        out_specs=(P("rep", None, None),) * 3 + (P("rep", "dp", None),) * 6,
        check_vma=False,
    )
```

```python
import functools

import jax
import jax.numpy as jnp
from jax import lax
from jax.experimental import pallas as pl
from jax.experimental.pallas import tpu as pltpu
from jax.sharding import PartitionSpec as P

MESH = pl.DeviceIdType.MESH
f32, bf16 = jnp.float32, jnp.bfloat16
T, D, F, LAYERS = 2048, 1024, 5120, 2
TILE = 256
STEPS = F // TILE
CHUNK = 5
PIECES = STEPS // CHUNK
WIDE = CHUNK * TILE
VMEM_LIMIT = 63 << 20
NT = (((1,), (1,)), ((), ()))
TN = (((0,), (0,)), ((), ()))


def dot(a, b):
    return jnp.dot(a, b, preferred_element_type=f32)


def dot_nt(a, b):
    return lax.dot_general(a, b, NT, preferred_element_type=f32)


def dot_tn(a, b):
    return lax.dot_general(a, b, TN, preferred_element_type=f32)


def normed(h):
    wide = h.astype(f32)
    scale = lax.rsqrt(jnp.mean(wide**2, -1, keepdims=True) + 1e-6)
    return (wide * scale).astype(bf16)


def up_kernel(x, wg, wu, a_out, act, a_scr):
    @pl.when(pl.program_id(0) == 0)
    def _():
        @pl.loop(0, T // 256)
        def _(m):
            s = pl.ds(m * 256, 256)
            a = normed(x[s, :])
            a_scr[s, :] = a
            a_out[s, :] = a

    def rows(m, _):
        s = pl.ds(m * 512, 512)
        gate, up = dot(a_scr[s, :], wg[...]), dot(a_scr[s, :], wu[...])
        act[s, :] = (jax.nn.silu(gate) * up).astype(bf16)
        return 0

    lax.fori_loop(0, T // 512, rows, 0, unroll=4)


def down_kernel(x, act, wd, h_out, a_out):
    h = x[...] + dot(act[...], wd[...]).astype(bf16)
    h_out[...] = h
    a_out[...] = normed(h)


def forward(x, wg, wu, wd):
    params = pltpu.CompilerParams(vmem_limit_bytes=VMEM_LIMIT)
    full = pl.BlockSpec((T, D), lambda j: (0, 0))
    columns = pl.BlockSpec((None, D, 512), lambda j: (0, 0, j))
    state, hidden = jax.ShapeDtypeStruct((T, D), bf16), jax.ShapeDtypeStruct((T, F), bf16)
    a0, act0 = pl.pallas_call(
        up_kernel,
        grid=(F // 512,),
        in_specs=[full, columns, columns],
        out_specs=[full, pl.BlockSpec((T, 512), lambda j: (0, j))],
        out_shape=[state, hidden],
        scratch_shapes=[pltpu.VMEM((T, D), bf16)],
        compiler_params=params,
        name="up",
    )(x, wg, wu)
    row = pl.BlockSpec((256, D), lambda m: (m, 0))
    whole = pl.BlockSpec((None, F, D), lambda m: (0, 0, 0), pipeline_mode=pl.Buffered(1))
    h1, a1 = pl.pallas_call(
        down_kernel,
        grid=(T // 256,),
        in_specs=[row, pl.BlockSpec((256, F), lambda m: (m, 0)), whole],
        out_specs=[row, row],
        out_shape=[state, state],
        compiler_params=params,
        name="down",
    )(x, act0, wd)
    return a0, act0, h1, a1


def index(x, y, z, c):
    return ((x * 2 + y) * 4 + z) * 2 + c


class Me:
    def __init__(self):
        d = lax.axis_index("dp")
        self.c = lax.rem(d, 2)
        self.z = lax.rem(lax.div(d, 2), 4)
        self.y = lax.rem(lax.div(d, 8), 2)
        self.x = lax.div(d, 16)
        self.core = index(self.x, self.y, self.z, 1 - self.c)
        self.xn = index(1 - self.x, self.y, self.z, self.c)
        self.yn = index(self.x, 1 - self.y, self.z, self.c)
        self.zn = {k: index(self.x, self.y, lax.rem(self.z + k, 4), self.c) for k in (1, 2, 3)}


def barrier(me):
    sem = pltpu.get_barrier_semaphore()
    peers = [me.core, me.xn, me.yn, *me.zn.values()]
    for peer in peers:
        pl.semaphore_signal(sem, inc=1, device_id=(0, peer), device_id_type=MESH)
    pl.semaphore_wait(sem, len(peers))


def pick(k, a, b):
    return (1 - k) * a + k * b


STAGES = ("s0", "s1", "s2", "s3", "s4", "g1", "g2", "g3", "g4")
KEYS = ("core", "xy1", "xy2", "z", "az", "axy1", "ac0", "axy2", "ac1", "ac2")


class Piece:
    def __init__(self, me, sems, layer, r, C, G, bufs, parts, tmp):
        self.me, self.l, self.r, self.C, self.G, self.parts, self.tmp = me, layer, r, C, G, parts, tmp
        self.R0, self.S0, self.R1, self.S1, self.R2, self.S2, self.R3 = bufs
        self.sems = {key: sems.take() for key in KEYS}

    def pairs(self, key):
        me, h = self.me, self.r // 2
        x, y, z, c = me.x, me.y, me.z, me.c
        if key == "core":
            return [(self.G.at[:, :, :, 1 - c], self.R0, me.core)]
        if key == "xy1":
            return [(self.S0.at[0], self.R1.at[0], me.xn), (self.S0.at[1], self.R1.at[1], me.yn)]
        if key == "xy2":
            return [(self.S1.at[0], self.R2.at[0], me.yn), (self.S1.at[1], self.R2.at[1], me.xn)]
        if key == "z":
            return [(self.S2.at[lax.rem(z + k, 4)], self.R3.at[k - 1], me.zn[k]) for k in (1, 2, 3)]
        out = []
        for part in self.parts:
            cols = pl.ds(part["block"] * part["width"], part["width"])
            lo, hi, both = pl.ds(0, h), pl.ds(h, h), pl.ds(0, self.r)

            def w(a, b, d, rows):
                return part["W"].at[self.l, a, b, d, c, rows, cols]

            every = slice(None)
            if key == "az":
                spots = [(w(x, y, z, both), me.zn[k]) for k in (1, 2, 3)]
            elif key == "axy1":
                spots = [(w(x, y, every, lo), me.yn), (w(x, y, every, hi), me.xn)]
            elif key == "ac0":
                spots = [(w(x, y, every, both), me.core)]
            elif key == "axy2":
                spots = [(w(x, every, every, lo), me.xn), (w(every, y, every, hi), me.yn)]
            elif key == "ac1":
                spots = [(w(x, 1 - y, every, lo), me.core), (w(1 - x, y, every, hi), me.core)]
            else:
                spots = [(w(1 - x, every, every, lo), me.core), (w(every, 1 - y, every, hi), me.core)]
            out += [(ref, ref, dev) for ref, dev in spots]
        return out

    def start(self, *keys):
        for key in keys:
            send, recv = self.sems[key]
            for src, dst, dev in self.pairs(key):
                pltpu.make_async_remote_copy(src_ref=src, dst_ref=dst, send_sem=send, recv_sem=recv, device_id=(0, dev), device_id_type=MESH).start()

    def whole(self, key):
        return {"core": self.R0, "z": self.R3, "az": self.R3, "xy1": self.R1, "axy2": self.R1, "ac2": self.R1}.get(key, self.R2)

    def wait(self, *keys, which=1):
        for key in keys:
            pltpu.make_async_copy(self.whole(key), self.whole(key), self.sems[key][which]).wait()

    def half(self, k):
        return pl.ds(k * (self.r // 2), self.r // 2)

    def add(self, terms, outs, key):
        V, sem = self.tmp["V"], self.tmp["sem"]
        n, flat = len(terms[0]), len(terms[0][0].shape) == 3
        a, b = (1, terms[0][0].shape[0]) if flat else terms[0][0].shape[:2]

        def view(i, k):
            return V.at[i, k, 0] if flat else V.at[i, k]

        for k in range(2):
            for i, term in enumerate(terms[k]):
                pltpu.make_async_copy(term, view(i, k), sem.at[k]).start()
        for k in range(2):
            all_of = V.at[pl.ds(0, n), k, pl.ds(0, a)]
            pltpu.make_async_copy(all_of, all_of, sem.at[k]).wait()

            @pl.loop(0, a * b)
            def _(j):
                q, d = j // b, lax.rem(j, b)
                total = V[0, k, q, d].astype(f32)
                for i in range(1, n):
                    total = total + V[i, k, q, d].astype(f32)
                V[4, k, q, d] = total.astype(bf16)

            pltpu.make_async_copy(view(4, k), outs[k], sem.at[2 + k]).start()
        for k in range(2):
            pltpu.make_async_copy(view(4, k), outs[k], sem.at[2 + k]).wait()
        self.start(key)

    def s0(self):
        self.start("core")

    def s1(self):
        me = self.me
        self.wait("core")
        G, R0, lo, hi = self.G, self.R0, self.half(0), self.half(1)
        self.add(
            [
                [G.at[1 - me.x, :, :, me.c, lo], R0.at[1 - me.x, :, :, lo]],
                [G.at[:, 1 - me.y, :, me.c, hi], R0.at[:, 1 - me.y, :, hi]],
            ],
            [self.S0.at[0], self.S0.at[1]],
            "xy1",
        )

    def s2(self):
        me = self.me
        self.wait("xy1")
        G, R0, R1, lo, hi = self.G, self.R0, self.R1, self.half(0), self.half(1)
        self.add(
            [
                [G.at[me.x, 1 - me.y, :, me.c, lo], R0.at[me.x, 1 - me.y, :, lo], R1.at[0, 1 - me.y]],
                [G.at[1 - me.x, me.y, :, me.c, hi], R0.at[1 - me.x, me.y, :, hi], R1.at[1, 1 - me.x]],
            ],
            [self.S1.at[0], self.S1.at[1]],
            "xy2",
        )

    def s3(self):
        me = self.me
        self.wait("xy2")
        x, y = me.x, me.y
        self.add(
            [
                [self.G.at[x, y, :, me.c, self.half(k)], self.R0.at[x, y, :, self.half(k)], self.R1.at[k, (y, x)[k]], self.R2.at[k]]
                for k in range(2)
            ],
            [self.S2.at[:, self.half(0)], self.S2.at[:, self.half(1)]],
            "z",
        )

    def s4(self):
        me, l, h = self.me, self.l, self.r // 2
        x, y, z, c = me.x, me.y, me.z, me.c
        self.wait("z")
        B, A, sem = self.tmp["B"], self.tmp["A"], self.tmp["sem"]
        width = self.C // len(self.parts)
        lo, hi = self.half(0), self.half(1)
        terms = [(self.G.at[x, y, z, c], B.at[0]), (self.R0.at[x, y, z], B.at[1]), (self.R3, B.at[pl.ds(4, 3)])]
        terms += [(self.R1.at[0, y, z], B.at[2, lo]), (self.R1.at[1, x, z], B.at[2, hi])]
        terms += [(self.R2.at[0, z], B.at[3, lo]), (self.R2.at[1, z], B.at[3, hi])]
        moments, w_out, out = [], [], []
        for p, part in enumerate(self.parts):
            there, here = pl.ds(part["block"] * width, width), pl.ds(p * width, width)
            terms += [(part["w"].at[l, x, y, z, c, :, there], B.at[7, :, here])]
            moments += [(part["m"].at[l, :, there], A.at[0, :, here]), (part["v"].at[l, :, there], A.at[1, :, here])]
            w_out += [(B.at[8, :, here], part["W"].at[l, x, y, z, c, :, there])]
            out += [(A.at[2, :, here], part["M"].at[l, :, there]), (A.at[3, :, here], part["V"].at[l, :, there])]

        def begin(pairs, i):
            for src, dst in pairs:
                pltpu.make_async_copy(src, dst, sem.at[i]).start()

        def end(ref, i):
            pltpu.make_async_copy(ref, ref, sem.at[i]).wait()

        begin(terms, 0)
        begin(moments, 1)
        end(B.at[pl.ds(0, 8)], 0)
        end(A.at[pl.ds(0, 2)], 1)
        blocks, across = self.r // 16, self.C // 512

        @pl.loop(0, blocks * across)
        def _(j):
            rows = pl.ds(pl.multiple_of(lax.rem(j, blocks) * 16, 16), 16)
            cols = pl.ds(pl.multiple_of(j // blocks * 512, 512), 512)
            t = B[0, rows, cols].astype(f32)
            for i in range(1, 7):
                t = t + B[i, rows, cols].astype(f32)
            t = t.astype(bf16).astype(f32)
            m = 0.9 * A[0, rows, cols] + 0.1 * t
            v = 0.95 * A[1, rows, cols] + 0.05 * t * t
            w = B[7, rows, cols].astype(f32)
            B[8, rows, cols] = (w - 0.02 * (m * lax.rsqrt(v + 1e-8) + 0.1 * w)).astype(bf16)
            A[2, rows, cols] = m
            A[3, rows, cols] = v

        begin(w_out, 2)
        begin(out, 3)
        end(B.at[8], 2)
        self.start("az")
        end(A.at[pl.ds(2, 2)], 3)

    def g1(self):
        self.wait("az")
        self.start("axy1", "ac0")

    def g2(self):
        self.wait("axy1")
        self.start("axy2", "ac1")

    def g3(self):
        self.wait("axy2")
        self.start("ac2")

    def g4(self):
        self.wait("ac0", "ac1", "ac2")
        self.wait(*KEYS, which=0)


class Sems:
    def __init__(self, send=None, recv=None):
        self.send, self.recv, self.n = send, recv, 0

    def take(self):
        self.n += 1
        return self.send.at[self.n - 1], self.recv.at[self.n - 1]


def buffers(r, C):
    h = r // 2
    shapes = (2, 2, 4, r, C), (2, 2, 4, h, C), (2, 2, 4, h, C), (2, 4, h, C), (2, 4, h, C), (4, r, C), (3, r, C)
    return [jax.ShapeDtypeStruct(s, bf16) for s in shapes]


HOSTS = (
    ("p1", 6.3, STEPS, [(CHUNK * (q + 1), [q]) for q in range(PIECES)]),
    ("p2", 3.1, 8, [(8, [4, 5])]),
    ("p3", 5.3, 10, []),
    ("p2", 3.1, 8, [(8, [6, 7])]),
    ("p1", 6.0, STEPS, [(CHUNK * (q + 1), [8 + q]) for q in range(PIECES)]),
)
COUNT = 12


def plan():
    cost = {"s0": 0.2, "s1": 3.6, "s2": 3.0, "s3": 2.9, "s4": 4.6, "g1": 0.2, "g2": 0.3, "g3": 0.3}
    links = {
        "s0": {"C": 5.2},
        "s1": {"X": 14.5, "Y": 14.5},
        "s2": {"X": 7.3, "Y": 7.3},
        "s3": {"Z": 14.5},
        "s4": {"Z": 14.5},
        "g1": {"X": 7.3, "Y": 7.3},
        "g2": {"X": 14.5, "Y": 14.5},
        "g3": {"C": 2.6},
    }
    now, free = 0.0, dict.fromkeys("XYZC", 0.0)
    done, ready = [0] * COUNT, [None] * COUNT
    last = len(STAGES) - 1

    def run(u):
        nonlocal now
        stage = STAGES[done[u]]
        now += cost[stage]
        end = now
        for link, span in links[stage].items():
            free[link] = max(now, free[link]) + span
            end = max(end, free[link])
        ready[u] = end + 2.5
        done[u] += 1
        return u, stage

    def candidates():
        c = [u for u in range(COUNT) if ready[u] is not None and done[u] < last and ready[u] <= now]
        return sorted(c, key=lambda u: (done[u] >= 4, u))

    schedule = []
    for _, span, steps, completes in HOSTS:
        slots = {}
        for s in range(steps):
            for at, pieces in completes:
                if at == s:
                    for u in pieces:
                        ready[u] = now
            while candidates():
                slots.setdefault(s, []).append(run(candidates()[0]))
            now += span
        for at, pieces in completes:
            if at == steps:
                for u in pieces:
                    ready[u] = now
        schedule.append(slots)
    tail = []
    while min(done) < last:
        u = (candidates() or [min((u for u in range(COUNT) if done[u] < last), key=lambda u: ready[u])])[0]
        now = max(now, ready[u])
        tail.append(run(u))
    return schedule, tail + [(u, "g4") for u in range(COUNT)]


def hidden_backward(layer, wg, wu, wd, keep, G, a_scr, dh_scr, gbuf, gsem, scratch, hook):
    def out_copies(i):
        q, col = i // CHUNK, lax.rem(i, CHUNK) * TILE
        return [
            pltpu.make_async_copy(gbuf.at[k], G.at[q, :, :, :, :, :, pl.ds(pl.multiple_of(k * WIDE + col, TILE), TILE)], gsem.at[k]) for k in range(2)
        ]

    def body(step, wg, wu, wd, *outs):
        i = step.index[0]
        act, dg, du = outs if keep else (None, *scratch)

        def rows(m, _):
            s = pl.ds(m * 512, 512)
            a = a_scr[s, :]
            gate, up, d = dot(a, wg[...]), dot(a, wu[...]), dot_nt(dh_scr[s, :], wd[...])
            d = d.astype(bf16).astype(f32)
            sig = 1.0 / (1.0 + jnp.exp(-gate))
            silu = gate * sig
            if keep:
                act[s, :] = (silu * up).astype(bf16)
            du[s, :] = (d * silu).astype(bf16)
            dg[s, :] = (d * up * (sig + silu * (1.0 - sig))).astype(bf16)
            return 0

        lax.fori_loop(0, T // 512, rows, 0, unroll=4)

        @pl.when(i > 0)
        def _():
            for copy in out_copies(i - 1):
                copy.wait()

        hook(i)
        gbuf[0] = dot_tn(a_scr[...], dg[...]).astype(bf16).reshape(gbuf.shape[1:])
        gbuf[1] = dot_tn(a_scr[...], du[...]).astype(bf16).reshape(gbuf.shape[1:])
        for copy in out_copies(i):
            copy.start()

    columns = pl.BlockSpec((None, D, TILE), lambda i: (layer, 0, i))
    tile = pl.BlockSpec((T, TILE), lambda i: (0, i))
    pltpu.emit_pipeline(
        body,
        grid=(STEPS,),
        in_specs=[columns, columns, pl.BlockSpec((None, TILE, D), lambda i: (layer, i, 0))],
        out_specs=[tile] * 3 if keep else [],
        _explicit_indices=True,
    )(wg, wu, wd, *(keep or ()))
    for copy in out_copies(STEPS - 1):
        copy.wait()


def down_gradient(act, Ga, Gb, dh_scr, hook):
    def body(step, act, ga, gb):
        hook(step.index[0])
        ga[...] = dot_tn(act[...], dh_scr[:, : D // 2]).astype(bf16).reshape(ga.shape)
        gb[...] = dot_tn(act[...], dh_scr[:, D // 2 :]).astype(bf16).reshape(gb.shape)

    out = pl.BlockSpec((None, None, 2, 2, 160, D // 2), lambda i: (i // 4, lax.rem(i // 2, 2), lax.rem(i, 2), 0, 0, 0))
    pltpu.emit_pipeline(
        body, grid=(8,), in_specs=[pl.BlockSpec((T, 640), lambda i: (0, i))], out_specs=[out, out], _explicit_indices=True
    )(act, Ga, Gb)


def state_gradient(layer, dg, du, wg, wu, acc, hook):
    def body(step, dg, du, wg, wu):
        i = step.index[0]
        hook(i)

        @pl.when(i == 0)
        def _():
            acc[...] = jnp.zeros_like(acc)

        for m in range(2):
            s = pl.ds(m * (T // 2), T // 2)
            acc[s, :] += dot_nt(dg[s, :], wg[...]) + dot_nt(du[s, :], wu[...])

    tile = pl.BlockSpec((T, 512), lambda i: (0, i))
    columns = pl.BlockSpec((None, D, 512), lambda i: (layer, 0, i))
    pltpu.emit_pipeline(body, grid=(F // 512,), in_specs=[tile, tile, columns, columns], _explicit_indices=True)(dg, du, wg, wu)


def through_norm(acc, h_scr, dh_scr):
    @pl.loop(0, T // 256)
    def _(m):
        s = pl.ds(m * 256, 256)
        da = acc[s, :].astype(bf16).astype(f32)
        wide = h_scr[s, :].astype(f32)
        scale = lax.rsqrt(jnp.mean(wide**2, -1, keepdims=True) + 1e-6)
        along = jnp.sum(da * wide, -1, keepdims=True) * (1.0 / D)
        d = da * scale - wide * (scale * scale * scale * along)
        dh_scr[s, :] = dh_scr[s, :] + d.astype(bf16)


def load(sems, *pairs):
    copies = [pltpu.make_async_copy(src, dst, sems.at[i]) for i, (src, dst) in enumerate(pairs)]
    for copy in copies:
        copy.start()
    for copy in copies:
        copy.wait()


def backward_kernel(sizes, *refs):
    (a0, act0, h1, a1, dy), w3, w7, m, v, refs = refs[:5], refs[5:8], refs[8:11], refs[11:14], refs[14:17], refs[17:]
    W, M, V, (act, dg, du), Gs, refs = refs[:3], refs[3:6], refs[6:9], refs[9:12], refs[12:18], refs[18:]
    bufs, refs = refs[: 7 * COUNT], refs[7 * COUNT :]
    send, recv, load_sem, gsem, work_sem, a_scr, dh_scr, acc, gbuf, dg_scr, du_scr, V_wide, B_wide, A_wide, V_down, B_down, A_down = refs
    G1, G1a, G1b, G0a, G0b, G0 = Gs
    me = Me()
    barrier(me)
    sems = Sems(send, recv)

    def part(i, block, width):
        return dict(w=w7[i], m=m[i], v=v[i], W=W[i], M=M[i], V=V[i], block=block, width=width)

    def piece(u, layer, r, C, G, parts, V, B, A):
        return Piece(me, sems, layer, r, C, G, bufs[7 * u : 7 * u + 7], parts, dict(V=V, B=B, A=A, sem=work_sem))

    def wide(u, layer, G, q):
        return piece(u, layer, sizes[0][0], 2 * WIDE, G.at[q], [part(0, q, WIDE), part(1, q, WIDE)], V_wide, B_wide, A_wide)

    def down(u, layer, G, q):
        return piece(u, layer, sizes[2][0], D // 2, G, [part(2, q, D // 2)], V_down, B_down, A_down)

    pieces = [wide(q, 1, G1, q) for q in range(4)] + [down(4, 1, G1a, 0), down(5, 1, G1b, 1)]
    pieces += [down(6, 0, G0a, 0), down(7, 0, G0b, 1)] + [wide(8 + q, 0, G0, q) for q in range(4)]
    schedule, tail = plan()

    def hook_of(host):
        def hook(i):
            for s, jobs in schedule[host].items():

                @pl.when(i == s)
                def _():
                    for u, stage in jobs:
                        getattr(pieces[u], stage)()

        return hook

    load(load_sem, (a1, a_scr), (dy, dh_scr))
    hidden_backward(1, *w3, (act, dg, du), G1, a_scr, dh_scr, gbuf, gsem, None, hook_of(0))
    down_gradient(act, G1a, G1b, dh_scr, hook_of(1))
    state_gradient(1, dg, du, w3[0], w3[1], acc, hook_of(2))
    load(load_sem, (h1, a_scr))
    through_norm(acc, a_scr, dh_scr)
    load(load_sem, (a0, a_scr))
    down_gradient(act0, G0a, G0b, dh_scr, hook_of(3))
    hidden_backward(0, *w3, None, G0, a_scr, dh_scr, gbuf, gsem, (dg_scr, du_scr), hook_of(4))
    for u, stage in tail:
        getattr(pieces[u], stage)()


def backward(sizes, a0, act0, h1, a1, dy, weights, m, v):
    hbm = pl.BlockSpec(memory_space=pl.ANY)

    def shape(s, dtype=bf16):
        return jax.ShapeDtypeStruct(s, dtype)

    views = [w.reshape(LAYERS, 2, 2, 4, 2, *s) for w, s in zip(weights, sizes, strict=True)]
    args = [a0, act0, h1, a1, dy, *weights, *views, *m, *v]
    outs = [shape(w.shape) for w in views] + [shape((LAYERS, *s), f32) for s in sizes] * 2 + [shape((T, F))] * 3
    wide, down = shape((PIECES, 2, 2, 4, 2, sizes[0][0], 2 * WIDE)), shape((2, 2, 4, 2, sizes[2][0], D // 2))
    outs += [wide, down, down, down, down, wide]
    for u in range(COUNT):
        outs += buffers(sizes[2][0], D // 2) if 4 <= u < 8 else buffers(sizes[0][0], 2 * WIDE)
    count = COUNT * len(KEYS)
    tokens = pltpu.VMEM((T, D), bf16)
    tile = pltpu.VMEM((T, TILE), bf16)

    def work(r, C):
        return pltpu.VMEM((5, 2, 2, 4, r // 2, C), bf16), pltpu.VMEM((9, r, C), bf16), pltpu.VMEM((4, r, C), f32)

    return pl.pallas_call(
        functools.partial(backward_kernel, sizes),
        out_shape=outs,
        in_specs=[hbm] * len(args),
        out_specs=[hbm] * len(outs),
        scratch_shapes=[
            pltpu.SemaphoreType.DMA((count,)),
            pltpu.SemaphoreType.DMA((count,)),
            pltpu.SemaphoreType.DMA((2,)),
            pltpu.SemaphoreType.DMA((2,)),
            pltpu.SemaphoreType.DMA((4,)),
            tokens,
            tokens,
            pltpu.VMEM((T, D), f32),
            pltpu.VMEM((2, 2, 2, 4, 2, sizes[0][0], TILE), bf16),
            tile,
            tile,
            *work(sizes[0][0], 2 * WIDE),
            *work(sizes[2][0], D // 2),
        ],
        compiler_params=pltpu.CompilerParams(collective_id=0, has_side_effects=True, vmem_limit_bytes=VMEM_LIMIT),
        name="backward",
    )(*args)


def solution(mesh):
    def step(x, dy, *arrays):
        weights, m, v = (arrays[i : i + 3] for i in (0, 3, 6))
        x, dy = x[0], dy[0]
        sizes = [t.shape[1:] for t in m]
        a0, act0, h1, a1 = forward(x, *weights)
        out = backward(sizes, a0, act0, h1, a1, dy, weights, m, v)
        return tuple(w.reshape(t.shape) for w, t in zip(out[:3], weights, strict=True)) + tuple(out[3:9])

    whole, rows, seq = P(None, None, None), P(None, "dp", None), P(("rep", "dp"), None, None)
    return jax.shard_map(
        step,
        mesh=mesh,
        in_specs=(seq, seq) + (whole,) * 3 + (rows,) * 6,
        out_specs=(P("rep", None, None),) * 3 + (P("rep", "dp", None),) * 6,
        check_vma=False,
    )
```

```python
import functools

import jax
import jax.numpy as jnp
from jax import lax
from jax.experimental import pallas as pl
from jax.experimental.pallas import tpu as pltpu
from jax.sharding import PartitionSpec as P

MESH = pl.DeviceIdType.MESH
f32, bf16 = jnp.float32, jnp.bfloat16
T, D, F, LAYERS = 2048, 1024, 5120, 2
TILE = 256
STEPS = F // TILE
CHIPS = (2, 2, 4)
N = None
EVERY = slice(None)
VMEM_LIMIT = 63 << 20
NT = (((1,), (1,)), ((), ()))
TN = (((0,), (0,)), ((), ()))


def dot(a, b):
    return jnp.dot(a, b, preferred_element_type=f32)


def dot_nt(a, b):
    return lax.dot_general(a, b, NT, preferred_element_type=f32)


def dot_tn(a, b):
    return lax.dot_general(a, b, TN, preferred_element_type=f32)


def normed(h):
    wide = h.astype(f32)
    scale = lax.rsqrt(jnp.mean(wide**2, -1, keepdims=True) + 1e-6)
    return (wide * scale).astype(bf16)


def forward(layer, x_in, wg, wu, wd, act, a, acc, h_scr, a_scr, sem):
    a_out = pltpu.make_async_copy(a_scr, a, sem)

    def body(step, wg, wu, wd, act):
        @pl.when(step.index[0] == 0)
        def _():
            x_in.wait()

            @pl.loop(0, T // 256)
            def _(m):
                s = pl.ds(m * 256, 256)
                a_scr[s, :] = normed(h_scr[s, :])
                acc[s, :] = jnp.zeros((256, D), f32)

            a_out.start()

        def rows(m, _):
            s = pl.ds(m * 512, 512)
            gate, up = dot(a_scr[s, :], wg[...]), dot(a_scr[s, :], wu[...])
            product = (gate * (1.0 / (1.0 + jnp.exp(-gate))) * up).astype(bf16)
            act[s, :] = product
            acc[s, :] += dot(product, wd[...])
            return 0

        lax.fori_loop(0, T // 512, rows, 0, unroll=4)

    columns = pl.BlockSpec((N, D, 512), lambda j: (layer, 0, j))
    pltpu.emit_pipeline(
        body,
        grid=(F // 512,),
        in_specs=[columns, columns, pl.BlockSpec((N, 512, D), lambda j: (layer, j, 0))],
        out_specs=[pl.BlockSpec((T, 512), lambda j: (0, j))],
        _explicit_indices=True,
    )(wg, wu, wd, act)
    a_out.wait()

    @pl.loop(0, T // 256)
    def _(m):
        s = pl.ds(m * 256, 256)
        h = h_scr[s, :] + acc[s, :].astype(bf16)
        h_scr[s, :] = h
        a_scr[s, :] = normed(h)


def index(x, y, z, c):
    return ((x * 2 + y) * 4 + z) * 2 + c


class Me:
    def __init__(self):
        d = lax.axis_index("dp")
        self.c = lax.rem(d, 2)
        self.z = lax.rem(lax.div(d, 2), 4)
        self.y = lax.rem(lax.div(d, 8), 2)
        self.x = lax.div(d, 16)
        self.inner = jnp.logical_and(self.z != 0, self.z != 3)
        self.core = index(self.x, self.y, self.z, 1 - self.c)
        self.xn = index(1 - self.x, self.y, self.z, self.c)
        self.yn = index(self.x, 1 - self.y, self.z, self.c)
        self.zn = {k: index(self.x, self.y, lax.rem(self.z + k, 4), self.c) for k in (1, 2, 3)}


def barrier(me):
    sem = pltpu.get_barrier_semaphore()
    peers = [me.core, me.xn, me.yn, *me.zn.values()]
    for peer in peers:
        pl.semaphore_signal(sem, inc=1, device_id=(0, peer), device_id_type=MESH)
    return functools.partial(pl.semaphore_wait, sem, len(peers))


def pick(k, a, b):
    return (1 - k) * a + k * b


KEYS = ("core", "xy1", "xy2", "z", "a1", "a2", "a21", "a22", "a23", "relay", "a3", "ac1", "ac2", "ac3")


class Piece:
    def __init__(self, me, sems, layer, r, C, G, first, bufs, parts, z_late, tmp):
        self.me, self.l, self.r, self.C, self.parts, self.z_late, self.tmp = me, layer, r, C, parts, z_late, tmp
        self.G, self.cols = G, pl.ds(first, C)
        self.R0, self.S0, self.R1, self.S1, self.R2, self.S2, self.R3 = bufs
        self.sems = {key: sems.take() for key in KEYS}
        sums = zip((self.s1, self.s2, self.s3, self.s4), ("core", "xy1", "xy2", "z"), strict=True)
        stages = [functools.partial(self.part, stage, key, i) for stage, key in sums for i in range(3)]
        self.stages = iter([self.s0, *stages, self.g1, *([self.g2] if z_late else []), self.g3, self.g4])

    def part(self, stage, key, i):
        if not i:
            self.wait(key)
        stage()[i]()

    def g(self, *spot):
        return self.G.at[(*spot, self.cols)]

    def pairs(self, key):
        me, h = self.me, self.r // 2
        x, y, z, c = me.x, me.y, me.z, me.c
        if key == "core":
            return [(self.g(EVERY, EVERY, EVERY, 1 - c, EVERY), self.R0, me.core)]
        if key == "xy1":
            return [(self.S0.at[0], self.R1.at[0], me.xn), (self.S0.at[1], self.R1.at[1], me.yn)]
        if key == "xy2":
            return [(self.S1.at[0], self.R2.at[0], me.yn), (self.S1.at[1], self.R2.at[1], me.xn)]
        if key == "z":
            return [(self.S2.at[lax.rem(z + k, 4)], self.R3.at[k - 1], me.zn[k]) for k in (1, 2, 3)]
        out = []
        for part in self.parts:
            cols = pl.ds(part["first"], part["width"])
            lo, hi = pl.ds(0, h), pl.ds(h, h)

            def w(a, b, d, rows):
                return part["W"].at[self.l, a, b, d, c, rows, cols]

            if key == "a1" and not self.z_late:
                spots = [(w(x, y, z, EVERY), me.zn[k]) for k in (1, 2, 3)]
            elif key == "a2":
                spots = [(w(x, y, EVERY, lo), me.yn), (w(x, y, EVERY, hi), me.xn)]
            elif key == "ac1":
                spots = [(w(x, y, EVERY, EVERY), me.core)]
            elif key == "ac2" and not self.z_late:
                spots = [(w(x, 1 - y, EVERY, lo), me.core), (w(1 - x, y, EVERY, hi), me.core)]
            elif key == "a1":
                spots = [(w(x, y, z, lo), me.yn), (w(x, y, z, hi), me.xn)]
            elif key[:2] == "a2":
                k = int(key[2])
                spots = [(w(x, EVERY, z, lo), me.zn[k]), (w(EVERY, y, z, hi), me.zn[k])]
            elif key == "relay":
                far, near = pick(z - 1, 3, 0), pick(z - 1, 0, 3)
                to = index(x, y, near, c)
                spots = [(w(x, EVERY, far, lo), to), (w(EVERY, y, far, hi), to)]
            elif key == "a3":
                spots = [(w(x, EVERY, EVERY, lo), me.xn), (w(EVERY, y, EVERY, hi), me.yn)]
            elif key == "ac2":
                spots = [(w(x, EVERY, EVERY, lo), me.core), (w(EVERY, y, EVERY, hi), me.core)]
            else:
                spots = [(w(1 - x, EVERY, EVERY, lo), me.core), (w(EVERY, 1 - y, EVERY, hi), me.core)]
            out += [(ref, ref, dev) for ref, dev in spots]
        return out

    def start(self, *keys):
        for key in keys:
            send, recv = self.sems[key]
            for src, dst, dev in self.pairs(key):
                pltpu.make_async_remote_copy(src_ref=src, dst_ref=dst, send_sem=send, recv_sem=recv, device_id=(0, dev), device_id_type=MESH).start()

    def whole(self, key):
        sizes = {"core": self.R0, "z": self.R3, "a1": self.R3.at[0], "xy1": self.R1, "xy2": self.R2, "ac2": self.R0.at[0]}
        if not self.z_late:
            sizes |= {"a1": self.R3, "a2": self.R2, "ac1": self.R2, "ac2": self.R2}
        if key in sizes:
            return sizes[key]
        return self.R3.at[pl.ds(0, 2)] if key[:2] in ("a2", "re") else self.R1

    def wait(self, *keys, which=1):
        for key in keys:
            pltpu.make_async_copy(self.whole(key), self.whole(key), self.sems[key][which]).wait()

    def half(self, k):
        return pl.ds(k * (self.r // 2), self.r // 2)

    def add(self, terms, outs, key):
        V, sem = self.tmp["V"], self.tmp["sem"]
        n, flat = len(terms[0]), len(terms[0][0].shape) == 3
        a, b = (1, terms[0][0].shape[0]) if flat else terms[0][0].shape[:2]
        cols = EVERY if self.C == V.shape[-1] else pl.ds(0, self.C)

        def spot(i):
            return (i // 2, i % 2) if flat else (i, EVERY)

        def view(i, k):
            return V.at[spot(i)[0], k, spot(i)[1], :, :, cols]

        out = 5 if flat else 2

        def stores():
            return [pltpu.make_async_copy(view(out, k), outs[k], sem.at[2 + k]) for k in range(2)]

        def load():
            for k in range(2):
                for i, term in enumerate(terms[k]):
                    pltpu.make_async_copy(term, view(i, k), sem.at[k]).start()

        def compute():
            for k in range(2):
                all_of = V.at[pl.ds(0, 3), k, 0, :, :, cols] if n == 3 else V.at[pl.ds(0, 2), k, :, :, :, cols]
                pltpu.make_async_copy(all_of, all_of, sem.at[k]).wait()

                @pl.loop(0, a * b)
                def _(j):
                    q, d = j // b, lax.rem(j, b)

                    def block(i):
                        return (i // 2, k, i % 2, j, EVERY, cols) if flat else (i, k, q, d, EVERY, cols)

                    total = V[block(0)].astype(f32)
                    for i in range(1, n):
                        total = total + V[block(i)].astype(f32)
                    V[block(out)] = total.astype(bf16)

                stores()[k].start()

        def send():
            for store in stores():
                store.wait()
            self.start(key)

        return load, compute, send

    def s0(self):
        self.start("core")

    def s1(self):
        me = self.me
        G, R0, lo, hi = self.g, self.R0, self.half(0), self.half(1)
        return self.add(
            [
                [G(1 - me.x, EVERY, EVERY, me.c, lo), R0.at[1 - me.x, :, :, lo]],
                [G(EVERY, 1 - me.y, EVERY, me.c, hi), R0.at[:, 1 - me.y, :, hi]],
            ],
            [self.S0.at[0], self.S0.at[1]],
            "xy1",
        )

    def s2(self):
        me = self.me
        G, R0, R1, lo, hi = self.g, self.R0, self.R1, self.half(0), self.half(1)
        return self.add(
            [
                [G(me.x, 1 - me.y, EVERY, me.c, lo), R0.at[me.x, 1 - me.y, :, lo], R1.at[0, 1 - me.y]],
                [G(1 - me.x, me.y, EVERY, me.c, hi), R0.at[1 - me.x, me.y, :, hi], R1.at[1, 1 - me.x]],
            ],
            [self.S1.at[0], self.S1.at[1]],
            "xy2",
        )

    def s3(self):
        me = self.me
        x, y = me.x, me.y
        return self.add(
            [
                [self.g(x, y, EVERY, me.c, self.half(k)), self.R0.at[x, y, :, self.half(k)], self.R1.at[k, (y, x)[k]], self.R2.at[k]]
                for k in range(2)
            ],
            [self.S2.at[:, self.half(0)], self.S2.at[:, self.half(1)]],
            "z",
        )

    def s4(self):
        me, l, h = self.me, self.l, self.r // 2
        x, y, z, c = me.x, me.y, me.z, me.c
        BB, AA, sem = self.tmp["B"], self.tmp["A"], self.tmp["sem"]
        width = self.C // len(self.parts)
        lo, hi = self.half(0), self.half(1)
        whole = self.C == BB.shape[-1]

        class At:
            def __init__(self, ref, C):
                self.ref, self.cols = ref, EVERY if whole else pl.ds(0, C)

            def at(self, *spot):
                spot += (EVERY,) * (2 - len(spot))
                return self.ref.at[spot if len(spot) == 3 else (*spot, self.cols)]

        B, A = At(BB, self.C).at, At(AA, self.C).at
        terms = [(self.g(x, y, z, c, EVERY), B(0)), (self.R0.at[x, y, z], B(1)), (self.R3, B(pl.ds(4, 3)))]
        terms += [(self.R1.at[0, y, z], B(2, lo)), (self.R1.at[1, x, z], B(2, hi))]
        terms += [(self.R2.at[0, z], B(3, lo)), (self.R2.at[1, z], B(3, hi))]
        moments, w_out, out = [], [], []
        for p, part in enumerate(self.parts):
            there, here = pl.ds(part["first"], width), pl.ds(p * width, width)
            terms += [(part["w"].at[l, x, y, z, c, :, there], B(7, EVERY, here))]
            moments += [(part["m"].at[l, :, there], A(0, EVERY, here)), (part["v"].at[l, :, there], A(1, EVERY, here))]
            w_out += [(B(8, EVERY, here), part["W"].at[l, x, y, z, c, :, there])]
            out += [(B(0, EVERY, here), part["g"].at[l, :, there])]

        def begin(pairs, i):
            for src, dst in pairs:
                pltpu.make_async_copy(src, dst, sem.at[i]).start()

        def end(ref, i):
            pltpu.make_async_copy(ref, ref, sem.at[i]).wait()

        def load():
            begin(terms, 4)
            begin(moments, 5)

        def compute():
            end(B(pl.ds(0, 8)), 4)
            end(A(pl.ds(0, 2)), 5)
            blocks, across = self.r // 16, self.C // 512

            @pl.loop(0, blocks * across)
            def _(j):
                rows = pl.ds(pl.multiple_of(lax.rem(j, blocks) * 16, 16), 16)
                cols = pl.ds(pl.multiple_of(j // blocks * 512, 512), 512)
                t = BB[0, rows, cols].astype(f32)
                for i in range(1, 7):
                    t = t + BB[i, rows, cols].astype(f32)
                t = t.astype(bf16)
                BB[0, rows, cols] = t
                t = t.astype(f32)
                m = 0.9 * AA[0, rows, cols] + 0.1 * t
                v = 0.95 * AA[1, rows, cols] + 0.05 * t * t
                w = BB[7, rows, cols].astype(f32)
                BB[8, rows, cols] = (w - 0.02 * (m * lax.rsqrt(v + 1e-8) + 0.1 * w)).astype(bf16)

            begin(w_out, 6)
            begin(out, 7)

        def send():
            end(B(8), 6)
            end(B(0), 7)
            self.start("a1")

        return load, compute, send

    def g1(self):
        self.wait("a1")
        if not self.z_late:
            self.start("a2", "ac1")
            return
        self.start("a22")
        pl.when(self.me.z != 3)(lambda: self.start("a21"))
        pl.when(self.me.z != 0)(lambda: self.start("a23"))

    def g2(self):
        self.wait("a22")
        pl.when(self.me.z != 0)(lambda: self.wait("a21"))
        pl.when(self.me.z != 3)(lambda: self.wait("a23"))
        pl.when(self.me.inner)(lambda: self.start("relay"))

    def g3(self):
        if self.z_late:
            pl.when(jnp.logical_not(self.me.inner))(lambda: self.wait("relay"))
        else:
            self.wait("a2")
        self.start("a3", "ac2")

    def g4(self):
        self.wait("a3")
        self.start("ac3")

    def end(self):
        self.wait("core", "xy1", "xy2", "z", "a1", "a3", "ac2", "ac3", which=0)
        self.wait("ac2", "ac3")
        if self.z_late:
            self.wait("a22", which=0)
            pl.when(self.me.z != 3)(lambda: self.wait("a21", which=0))
            pl.when(self.me.z != 0)(lambda: self.wait("a23", which=0))
            pl.when(self.me.inner)(lambda: self.wait("relay", which=0))
        else:
            self.wait("ac1")
            self.wait("a2", "ac1", which=0)


class Sems:
    def __init__(self, send=None, recv=None):
        self.send, self.recv, self.n = send, recv, 0

    def take(self):
        self.n += 1
        return self.send.at[self.n - 1], self.recv.at[self.n - 1]


def buffers(r, C):
    h = r // 2
    quarter, eighth = (*CHIPS, h, C), (*CHIPS[1:], h, C)
    shapes = (*CHIPS, r, C), quarter, quarter, eighth, eighth, (4, r, C), (3, r, C)
    return [jax.ShapeDtypeStruct(s, bf16) for s in shapes]


WIDE_1 = (2, 4, 4, 5, 5)
WIDE_0 = (5, 5, 5, 3, 2)
Z_LATE = "-----zz-z--zzz"
PLAN = (
    ("----a--a-a-a---a-ab-a-b-b-ba-a-a--c-ab-ab-abc-cc-ab-b-b--c-c", "dac-b-bd-bda-dc-cc--b--d",),
    ("bdec-dcc--e-be-e-cd-d",),
    ("gfde-ec-eg-ggfd-fdcf-de-e-e-g-gdg",),
    ("def-effeg-gg---d-e",),
    ("eifh-gffgg-i-i-eih-ghhf-ff---i-ji-i-g-jh-jhfhj-gi-i-ih-hh--k", "-fj-j-jk-kfk-gi-i-ij-j-hj-lhh-f-l-ll-j-kjkijk-m-h-mmml-ll",),
)
TAIL = ("nkkknnhinmimmjlllkhkknnnlllimmkmjnnlnmmmkjmlnnnlknmmnlnmn",)
COUNT = len(WIDE_1) + len(WIDE_0) + 4


def starts(sizes):
    return [sum(sizes[:q]) for q in range(len(sizes))]


def hidden_backward(layer, sizes, wg, wu, wd, keep, G, a_scr, dh_scr, gbuf, gsem, scratch, hook):
    def out_copies(i):
        first = size = 0
        for start, n in zip(starts(sizes), sizes, strict=True):
            first, size = jnp.where(i >= start, start, first), jnp.where(i >= start, n, size)
        return [
            pltpu.make_async_copy(gbuf.at[k], G.at[:, :, :, :, :, pl.ds(pl.multiple_of((i + first + k * size) * TILE, TILE), TILE)], gsem.at[k])
            for k in range(2)
        ]

    def body(step, wg, wu, wd, *outs):
        i = step.index[0]
        act, dg, du = outs if keep else (None, *scratch)

        def rows(m, _):
            s = pl.ds(m * 512, 512)
            a = a_scr[s, :]
            gate, up, d = dot(a, wg[...]), dot(a, wu[...]), dot_nt(dh_scr[s, :], wd[...])
            d = d.astype(bf16).astype(f32)
            sig = 1.0 / (1.0 + jnp.exp(-gate))
            silu = gate * sig
            if keep:
                act[s, :] = (silu * up).astype(bf16)
            du[s, :] = (d * silu).astype(bf16)
            dg[s, :] = (d * up * (sig + silu * (1.0 - sig))).astype(bf16)
            return 0

        lax.fori_loop(0, T // 512, rows, 0, unroll=4)

        @pl.when(i > 0)
        def _():
            for copy in out_copies(i - 1):
                copy.wait()

        hook(i, 0, 2)
        gbuf[0] = dot_tn(a_scr[...], dg[...]).astype(bf16).reshape(gbuf.shape[1:])
        gbuf[1] = dot_tn(a_scr[...], du[...]).astype(bf16).reshape(gbuf.shape[1:])
        for copy in out_copies(i):
            copy.start()
        hook(i, 1, 2)

    columns = pl.BlockSpec((N, D, TILE), lambda i: (layer, 0, i))
    tile = pl.BlockSpec((T, TILE), lambda i: (0, i))
    pltpu.emit_pipeline(
        body,
        grid=(STEPS,),
        in_specs=[columns, columns, pl.BlockSpec((N, TILE, D), lambda i: (layer, i, 0))],
        out_specs=[tile] * 3 if keep else [],
        _explicit_indices=True,
    )(wg, wu, wd, *(keep or ()))
    for copy in out_copies(STEPS - 1):
        copy.wait()


def down_gradient(act, G, dh_scr, hook):
    def body(step, act, g):
        @pl.loop(0, 2)
        def _(k):
            cols = pl.ds(pl.multiple_of(k * (D // 2), D // 2), D // 2)
            g[k] = dot_tn(act[...], dh_scr[:, cols]).astype(bf16).reshape(g.shape[1:])

        hook(step.index[0])

    out = pl.BlockSpec((2, N, N, 2, 2, 160, D // 2), lambda i: (0, i // 4, lax.rem(i // 2, 2), lax.rem(i, 2), 0, 0, 0))
    pltpu.emit_pipeline(
        body, grid=(8,), in_specs=[pl.BlockSpec((T, 640), lambda i: (0, i))], out_specs=[out], _explicit_indices=True
    )(act, G)


def state_gradient(layer, dg, du, wg, wu, acc, hook):
    def body(step, dg, du, wg, wu):
        i = step.index[0]

        @pl.when(i == 0)
        def _():
            acc[...] = jnp.zeros_like(acc)

        @pl.loop(0, 2)
        def _(m):
            s = pl.ds(m * (T // 2), T // 2)
            acc[s, :] += dot_nt(dg[s, :], wg[...]) + dot_nt(du[s, :], wu[...])

        hook(i)

    tile = pl.BlockSpec((T, 512), lambda i: (0, i))
    columns = pl.BlockSpec((N, D, 512), lambda i: (layer, 0, i))
    pltpu.emit_pipeline(body, grid=(F // 512,), in_specs=[tile, tile, columns, columns], _explicit_indices=True)(dg, du, wg, wu)


def through_norm(acc, h_scr, dh_scr):
    @pl.loop(0, T // 256)
    def _(m):
        s = pl.ds(m * 256, 256)
        da = acc[s, :].astype(bf16).astype(f32)
        wide = h_scr[s, :].astype(f32)
        scale = lax.rsqrt(jnp.mean(wide**2, -1, keepdims=True) + 1e-6)
        along = jnp.sum(da * wide, -1, keepdims=True) * (1.0 / D)
        d = da * scale - wide * (scale * scale * scale * along)
        dh_scr[s, :] = dh_scr[s, :] + d.astype(bf16)


def step_kernel(sizes, *refs):
    (x, dy), w3, w7, m, v, refs = refs[:2], refs[2:5], refs[5:8], refs[8:11], refs[11:14], refs[14:]
    W, g, (a0, act0, act, dg, du), Gs, refs = refs[:3], refs[3:6], refs[6:11], refs[11:15], refs[15:]
    bufs, refs = refs[: 7 * COUNT], refs[7 * COUNT :]
    send, recv, load_sem, gsem, work_sem, a_scr, h_scr, dh_scr, acc, gbuf, dg_scr, du_scr, V_wide, B_wide, A_wide, V_down, B_down, A_down = refs
    G1, G1d, G0d, G0 = Gs
    me = Me()
    arrived = barrier(me)
    sems = Sems(send, recv)

    def part(i, first, width):
        return dict(w=w7[i], m=m[i], v=v[i], W=W[i], g=g[i], first=first, width=width)

    def piece(layer, r, C, G, first, parts, V, B, A):
        u = len(pieces)
        work = dict(V=V, B=B, A=A, sem=work_sem.at[pl.ds(0 if V is V_wide else 8, 8)])
        pieces.append(Piece(me, sems, layer, r, C, G, first, bufs[7 * u : 7 * u + 7], parts, Z_LATE[u] == "z", work))

    def wide_pieces(layer, tiles, G):
        for start, n in zip(starts(tiles), tiles, strict=True):
            parts = [part(i, start * TILE, n * TILE) for i in range(2)]
            piece(layer, sizes[0][0], 2 * n * TILE, G, 2 * start * TILE, parts, V_wide, B_wide, A_wide)

    def down_pieces(layer, G):
        for q in range(2):
            piece(layer, sizes[2][0], D // 2, G.at[q], 0, [part(2, q * (D // 2), D // 2)], V_down, B_down, A_down)

    pieces = []
    wide_pieces(1, WIDE_1, G1)
    down_pieces(1, G1d)
    down_pieces(0, G0d)
    wide_pieces(0, WIDE_0, G0)

    plan = [
        [[next(pieces[ord(letter) - ord("a")].stages) for letter in letters] for letters in "".join(host).split("-")]
        for host in (*PLAN, TAIL)
    ]

    def run(stages):
        for stage in stages:
            stage()

    def hook_of(host):
        def among(i, jobs):
            if len(jobs) > 1:
                middle = jobs[len(jobs) // 2][0]
                pl.when(i < middle)(lambda: among(i, jobs[: len(jobs) // 2]))
                pl.when(i >= middle)(lambda: among(i, jobs[len(jobs) // 2 :]))
            elif jobs:
                pl.when(i == jobs[0][0])(lambda: run(jobs[0][1]))

        def hook(i, place=0, places=1):
            among(i, [job for job in enumerate(plan[host][place::places]) if job[1]])

        return hook

    x_in = pltpu.make_async_copy(x, h_scr, load_sem.at[0])
    dy_in = pltpu.make_async_copy(dy, dh_scr, load_sem.at[1])
    x_in.start()
    dy_in.start()
    forward(0, x_in, *w3, act0, a0, acc, h_scr, a_scr, load_sem.at[2])
    dy_in.wait()
    arrived()
    hidden_backward(1, WIDE_1, *w3, (act, dg, du), G1, a_scr, dh_scr, gbuf, gsem, None, hook_of(0))
    a0_in = pltpu.make_async_copy(a0, a_scr, load_sem.at[0])
    a0_in.start()
    down_gradient(act, G1d, dh_scr, hook_of(1))
    state_gradient(1, dg, du, w3[0], w3[1], acc, hook_of(2))
    through_norm(acc, h_scr, dh_scr)
    a0_in.wait()
    down_gradient(act0, G0d, dh_scr, hook_of(3))
    hidden_backward(0, WIDE_0, *w3, None, G0, a_scr, dh_scr, gbuf, gsem, (dg_scr, du_scr), hook_of(4))
    run(*plan[-1])
    for one in pieces:
        one.end()


def run_step(sizes, x, dy, weights, m, v):
    hbm = pl.BlockSpec(memory_space=pl.ANY)

    def shape(s, dtype=bf16):
        return jax.ShapeDtypeStruct(s, dtype)

    views = [w.reshape(LAYERS, *CHIPS, 2, *s) for w, s in zip(weights, sizes, strict=True)]
    args = [x, dy, *weights, *views, *m, *v]
    outs = [shape(w.shape) for w in views] + [shape((LAYERS, *s)) for s in sizes] + [shape((T, D))] + [shape((T, F))] * 4
    wide, down = shape((*CHIPS, 2, sizes[0][0], 2 * F)), shape((2, *CHIPS, 2, sizes[2][0], D // 2))
    outs += [wide, down, down, wide]
    for n in (*WIDE_1, 0, 0, 0, 0, *WIDE_0):
        outs += buffers(sizes[0][0], 2 * n * TILE) if n else buffers(sizes[2][0], D // 2)
    count = COUNT * len(KEYS)
    tokens = pltpu.VMEM((T, D), bf16)
    tile = pltpu.VMEM((T, TILE), bf16)

    def work(r, C):
        return pltpu.VMEM((3, *CHIPS, r // 2, C), bf16), pltpu.VMEM((9, r, C), bf16), pltpu.VMEM((2, r, C), f32)

    return pl.pallas_call(
        functools.partial(step_kernel, sizes),
        out_shape=outs,
        in_specs=[hbm] * len(args),
        out_specs=[hbm] * len(outs),
        scratch_shapes=[
            pltpu.SemaphoreType.DMA((count,)),
            pltpu.SemaphoreType.DMA((count,)),
            pltpu.SemaphoreType.DMA((3,)),
            pltpu.SemaphoreType.DMA((2,)),
            pltpu.SemaphoreType.DMA((16,)),
            tokens,
            tokens,
            tokens,
            pltpu.VMEM((T, D), f32),
            pltpu.VMEM((2, *CHIPS, 2, sizes[0][0], TILE), bf16),
            tile,
            tile,
            *work(sizes[0][0], 2 * max(WIDE_1 + WIDE_0) * TILE),
            *work(sizes[2][0], D // 2),
        ],
        compiler_params=pltpu.CompilerParams(collective_id=0, has_side_effects=True, vmem_limit_bytes=VMEM_LIMIT),
        name="step",
    )(*args)


def solution(mesh):
    def step(x, dy, *arrays):
        weights, m, v = (arrays[i : i + 3] for i in (0, 3, 6))
        x, dy = x[0], dy[0]
        sizes = [t.shape[1:] for t in m]
        out = run_step(sizes, x, dy, weights, m, v)
        g = [t.astype(f32) for t in out[3:6]]
        new_m = [0.9 * m + 0.1 * g for m, g in zip(m, g, strict=True)]
        new_v = [0.95 * v + 0.05 * g * g for v, g in zip(v, g, strict=True)]
        return (*(w.reshape(t.shape) for w, t in zip(out[:3], weights, strict=True)), *new_m, *new_v)

    whole, rows, seq = P(None, None, None), P(None, "dp", None), P(("rep", "dp"), None, None)
    return jax.shard_map(
        step,
        mesh=mesh,
        in_specs=(seq, seq) + (whole,) * 3 + (rows,) * 6,
        out_specs=(P("rep", None, None),) * 3 + (P("rep", "dp", None),) * 6,
        check_vma=False,
    )
```
